32 devices in a mesh: energy: 8 (over y, x, core), cell: 4 (over z).
Axes of the slice: x: 2, y: 2, z: 4, core: 2. Of those that a mesh axis runs over, the one named last changes fastest.
Arguments:
- g_retarded: bfloat16 [2, 8, 4, 128, 512], P(None, 'energy', None, None, 'cell'), may hold values from -0.75 to 0.75
- sigma_lesser: bfloat16 [2, 8, 128, 512], P(None, 'energy', None, 'cell'), may hold values from -1.5 to 1.5
- w_screened: bfloat16 [2, 8, 4, 128, 512], P(None, 'energy', None, None, 'cell'), may hold values from -0.75 to 0.75
- coupling: int32 [4, 4], replicated, may hold values 0 or 1
Outputs:
- polarization: bfloat16 [4, 2, 8, 16384], P('cell', None, 'energy')
- w_lesser: bfloat16 [4, 2, 8, 128, 128], P('cell', None, 'energy')
The draws below stay inside these ranges and needn't reach their ends.
Inputs may be any that keep to these rules, and one draw needn't show every extreme that they name: coupling[i, j] is 1 where cell i is coupled to cell j and 0 elsewhere.
All inputs are finite; a program needn't handle non-finite values.
Results may differ from the reference program's by a relative error of at most 0.024.
Values may be sent and summed in bfloat16 or wider, within the bound.
No kernel may reach another device: no remote copies, remote signals or barrier semaphores. Data moves between devices by JAX's collectives and lax.ppermute only.
A program may use at most 64 MiB of HBM per device.

```python
import math
import jax
import jax.numpy as jnp
from jax import lax

ORB = 128
CELL_DEV = 1
NCELLS = 4
ENERGIES = 8
N_CELL = 4


def set_ends(values, rng, low, high):
    longest = values.shape.index(max(values.shape))
    spots = []
    for shift in (0, 1):
        where = [jax.random.randint(jax.random.fold_in(rng, axis), (), 0, length) for axis, length in enumerate(values.shape)]
        where[longest] = (where[longest] + shift) % values.shape[longest]
        spots.append(tuple(where))
    return values.at[spots[0]].set(low).at[spots[1]].set(high)


def with_spikes(result, rng, source, target, blocks, factor):
    def block_of(position):
        return (jnp.arange(result.shape[position]) // (result.shape[position] // blocks)).reshape((-1,) + (1,) * (result.ndim - 1 - position))

    one_side = jax.random.permutation(rng, blocks)[block_of(target)]
    second = (block_of(target) + blocks // 2) % blocks
    return jnp.where((block_of(source) == one_side) | (block_of(source) == second), factor * result, result)


def level_of(own_key, shape, shards, least, top_value):
    loudness = 1.0
    for axis_at, shards_of in shards:
        draws = jax.random.uniform(jax.random.fold_in(jax.random.fold_in(own_key, 6), axis_at), (shards_of,), jnp.float32, least / len(shards), top_value / len(shards))
        loudness = loudness * jnp.repeat(jnp.exp(draws), shape[axis_at] // shards_of).reshape((-1,) + (1,) * (len(shape) - 1 - axis_at))
    return loudness


def normal_values(key, dims, width, limit, split=(), held_as=jnp.bfloat16):
    gain = level_of(key, dims, split, -0.22, 0.18) if split else 1.0
    values = jax.random.normal(key, dims, jnp.float32) * width * gain
    return jnp.minimum(jnp.maximum(values, -limit), limit).astype(held_as)


def noise_with(own_key, shape, scale, bound, pieces, heavy, held_as=jnp.bfloat16):
    drawn = scale * jax.random.normal(own_key, shape, jnp.float32)
    if pieces:
        drawn = drawn * level_of(own_key, shape, pieces, -0.22, 0.18)
    return jnp.clip(with_spikes(drawn, jax.random.fold_in(own_key, 3), *heavy), -bound, bound).astype(held_as)


def setup_inputs(seed: int = 0) -> dict:
    key_of = jax.random.split(jax.random.key(seed), 5)
    g_retarded = noise_with(key_of[0], (2, ENERGIES, NCELLS, ORB, NCELLS * ORB), ORB ** -0.5, 0.75, ((1, 8), (4, 4)), (4, 2, 4, 2.0))
    sigma_lesser = normal_values(key_of[1], (2, ENERGIES, ORB, NCELLS * ORB), 0.25, 1.5, ((1, 8), (3, 4)))
    w_screened = noise_with(key_of[2], (2, ENERGIES, NCELLS, ORB, NCELLS * ORB), ORB ** -0.5, 0.75, ((1, 8), (4, 4)), (4, 2, 4, 2.0))
    coupling = set_ends((jax.random.randint(key_of[3], (NCELLS, NCELLS), 0, 2) < 1).astype(jnp.int32), jax.random.fold_in(key_of[3], 1), 0, 1)
    return dict(g_retarded=g_retarded, sigma_lesser=sigma_lesser, w_screened=w_screened, coupling=coupling)


def to_half(value):
    return lax.optimization_barrier(value.astype(jnp.bfloat16)).astype(jnp.float32)

def sandwich(columns, sources, coupling):
    energies = columns.shape[1]
    source = sources.astype(jnp.float32).reshape(2, energies, ORB, NCELLS, ORB)
    src_re = source[0]
    src_im = source[1]
    weights = coupling.astype(jnp.float32)

    def one_row(row_index):
        block = lax.dynamic_index_in_dim(columns, row_index, 2, keepdims=False)
        block = block.astype(jnp.float32).reshape(2, energies, ORB, NCELLS, ORB)
        col_re = block[0]
        col_im = block[1]
        mid_re = jnp.einsum('ebjc,ecjd->ebjd', col_re, src_re) - jnp.einsum('ebjc,ecjd->ebjd', col_im, src_im)
        mid_im = jnp.einsum('ebjc,ecjd->ebjd', col_re, src_im) + jnp.einsum('ebjc,ecjd->ebjd', col_im, src_re)
        mid_re = to_half(mid_re)
        mid_im = to_half(mid_im)
        part_re = jnp.einsum('ebjc,edjc->ejbd', mid_re, col_re) + jnp.einsum('ebjc,edjc->ejbd', mid_im, col_im)
        part_im = jnp.einsum('ebjc,edjc->ejbd', mid_im, col_re) - jnp.einsum('ebjc,edjc->ejbd', mid_re, col_im)
        row_weight = weights[row_index][None, :, None, None]
        part_re = (part_re * row_weight).reshape(energies, N_CELL, CELL_DEV, ORB, ORB).sum(axis=2)
        part_im = (part_im * row_weight).reshape(energies, N_CELL, CELL_DEV, ORB, ORB).sum(axis=2)
        total_re = to_half(part_re).sum(axis=1)
        total_im = to_half(part_im).sum(axis=1)
        return jnp.stack([total_re, total_im], axis=0)
    return lax.map(one_row, jnp.arange(NCELLS, dtype=jnp.int32))

def diagonal_blocks(columns):
    energies = columns.shape[1]

    def one_block(row_index):
        start = (jnp.zeros((), jnp.int32), jnp.zeros((), jnp.int32), row_index, jnp.zeros((), jnp.int32), (row_index * ORB).astype(jnp.int32))
        block = lax.dynamic_slice(columns, start, (2, energies, 1, ORB, ORB))
        return block[:, :, 0].astype(jnp.float32)
    return lax.map(one_block, jnp.arange(NCELLS, dtype=jnp.int32))

def reference(g_retarded, sigma_lesser, w_screened, coupling):
    lesser = sandwich(g_retarded, sigma_lesser, coupling)
    diagonal = diagonal_blocks(g_retarded)
    diag_re = diagonal[:, 0]
    diag_im = diagonal[:, 1]
    greater = lesser + jnp.stack([diag_re - jnp.swapaxes(diag_re, -1, -2), diag_im + jnp.swapaxes(diag_im, -1, -2)], axis=1)
    lesser_half = lesser.astype(jnp.bfloat16).astype(jnp.float32)
    greater_half = greater.astype(jnp.bfloat16).astype(jnp.float32)
    lesser_complex = lesser_half[:, 0] + 1j * lesser_half[:, 1]
    greater_complex = greater_half[:, 0] + 1j * greater_half[:, 1]
    spec_lesser = jnp.fft.fft(lesser_complex, n=2 * ENERGIES, axis=1)
    spec_greater = jnp.fft.fft(greater_complex, n=2 * ENERGIES, axis=1)
    correlation = jnp.fft.ifft(spec_lesser * jnp.conj(spec_greater), axis=1)[:, :ENERGIES]
    polar = -1j / math.sqrt(ENERGIES) * correlation
    polar_half = jnp.stack([jnp.real(polar), jnp.imag(polar)], axis=1).astype(jnp.bfloat16)
    sources = jnp.transpose(polar_half, (1, 2, 3, 0, 4)).reshape(2, ENERGIES, ORB, NCELLS * ORB)
    screened = sandwich(w_screened, sources, coupling)
    polarization = polar_half.reshape(NCELLS, 2, ENERGIES, ORB * ORB)
    return (polarization, screened.astype(jnp.bfloat16))
```

```python
import functools
import math

import jax
import jax.numpy as jnp
from jax import lax
from jax.experimental import pallas as pl
from jax.experimental.pallas import tpu as pltpu
from jax.sharding import PartitionSpec as P

VMEM = pltpu.MemorySpace.VMEM
SMEM = pltpu.MemorySpace.SMEM


def call(body, out_shape, spaces):
    outs = out_shape if isinstance(out_shape, (tuple, list)) else (out_shape,)
    out_specs = [pl.BlockSpec(memory_space=VMEM) for _ in outs]
    return pl.pallas_call(
        body,
        out_shape=out_shape,
        in_specs=[pl.BlockSpec(memory_space=space) for space in spaces],
        out_specs=out_specs if isinstance(out_shape, (tuple, list)) else out_specs[0],
    )


def source_matrix(src_re, src_im):
    return jnp.concatenate(
        [
            jnp.concatenate([src_re, src_im], axis=1),
            jnp.concatenate([-src_im, src_re], axis=1),
        ],
        axis=0,
    )


def sandwich_block(block, source):
    half = block.shape[0]
    mid = jnp.dot(block, source, preferred_element_type=jnp.float32).astype(jnp.bfloat16)
    turned = jnp.concatenate([mid[:, half:], -mid[:, :half]], axis=1)
    left = jnp.concatenate([mid, turned], axis=0)
    return lax.dot_general(
        left, block, (((1,), (1,)), ((), ())), preferred_element_type=jnp.float32
    )


def lesser_kernel(coupling, green, sigma, chunks, spectral):
    cell = lax.axis_index("cell")
    owners, cells, _, rows, _ = chunks.shape
    orbitals = owners * rows
    source = source_matrix(sigma[0, 0], sigma[1, 0])
    diag_re = green[0, 0, cell].astype(jnp.float32)
    diag_im = green[1, 0, cell].astype(jnp.float32)
    diff_re = (diag_re - diag_re.T).astype(jnp.bfloat16)
    diff_im = (diag_im + diag_im.T).astype(jnp.bfloat16)
    for owner in range(owners):
        here = slice(owner * rows, (owner + 1) * rows)
        spectral[owner, 0] = diff_re[here]
        spectral[owner, 1] = diff_im[here]
    for i in range(cells):
        block = jnp.concatenate([green[0, 0, i], green[1, 0, i]], axis=1)
        part = sandwich_block(block, source)
        part = (part * coupling[i, cell].astype(jnp.float32)).astype(jnp.bfloat16)
        for owner in range(owners):
            for c in range(2):
                start = c * orbitals + owner * rows
                chunks[owner, i, c] = part[start : start + rows]


def correlate_kernel(chunks, spectral, polar):
    energies, cells = chunks.shape[0], chunks.shape[1]
    scale = 1.0 / math.sqrt(energies)
    lesser, greater = [], []
    for e in range(energies):
        low, high = [], []
        for c in range(2):
            total = chunks[e, 0, c].astype(jnp.float32)
            for j in range(1, cells):
                total = total + chunks[e, j, c].astype(jnp.float32)
            above = total + spectral[e, c].astype(jnp.float32)
            low.append(total.astype(jnp.bfloat16).astype(jnp.float32))
            high.append(above.astype(jnp.bfloat16).astype(jnp.float32))
        lesser.append(low)
        greater.append(high)
    for w in range(energies):
        real = imag = None
        for e in range(energies - w):
            low_re, low_im = lesser[e + w]
            high_re, high_im = greater[e]
            re = low_im * high_re - low_re * high_im
            im = low_re * high_re + low_im * high_im
            real = re if real is None else real + re
            imag = im if imag is None else imag + im
        polar[w, 0] = (real * scale).astype(jnp.bfloat16)
        polar[w, 1] = (imag * -scale).astype(jnp.bfloat16)


def screened_kernel(coupling, screen, rows, polar, partial):
    cell = lax.axis_index("cell")
    owners, _, height, width = rows.shape
    cells = screen.shape[2]
    parts = [rows[:, c].reshape(owners * height, width) for c in range(2)]
    polar[0] = parts[0]
    polar[1] = parts[1]
    source = source_matrix(*parts)
    for i in range(cells):
        block = jnp.concatenate([screen[0, 0, i], screen[1, 0, i]], axis=1)
        part = sandwich_block(block, source)
        part = (part * coupling[i, cell].astype(jnp.float32)).astype(jnp.bfloat16)
        partial[i, 0] = part[:width]
        partial[i, 1] = part[width:]


def on_device(g_retarded, sigma_lesser, w_screened, coupling):
    owners = lax.axis_size("energy")
    cells = lax.axis_size("cell")
    orbitals = sigma_lesser.shape[2]
    rows = orbitals // owners
    half = functools.partial(jax.ShapeDtypeStruct, dtype=jnp.bfloat16)
    chunks, spectral = call(
        lesser_kernel,
        (half((owners, cells, 2, rows, orbitals)), half((owners, 2, rows, orbitals))),
        (SMEM, VMEM, VMEM),
    )(coupling, g_retarded, sigma_lesser)
    spectral = lax.all_to_all(spectral, "energy", 0, 0, tiled=True)
    chunks = lax.all_to_all(
        chunks.reshape(owners * cells, 2, rows, orbitals), ("energy", "cell"), 0, 0, tiled=True
    ).reshape(owners, cells, 2, rows, orbitals)
    polar = call(correlate_kernel, half((owners, 2, rows, orbitals)), (VMEM, VMEM))(
        chunks, spectral
    )
    polar = lax.all_to_all(polar, "energy", 0, 0, tiled=True)
    polar, partial = call(
        screened_kernel,
        (half((2, orbitals, orbitals)), half((cells, 2, orbitals, orbitals))),
        (SMEM, VMEM, VMEM),
    )(coupling, w_screened, polar)
    partial = lax.all_to_all(partial, "cell", 0, 0, tiled=True)
    screened = partial.astype(jnp.float32).sum(axis=0).astype(jnp.bfloat16)
    return (
        polar.reshape(1, 2, 1, orbitals * orbitals),
        screened.reshape(1, 2, 1, orbitals, orbitals),
    )


def solution(mesh):
    return jax.shard_map(
        on_device,
        mesh=mesh,
        in_specs=(
            P(None, "energy", None, None, "cell"),
            P(None, "energy", None, "cell"),
            P(None, "energy", None, None, "cell"),
            P(),
        ),
        out_specs=(P("cell", None, "energy", None), P("cell", None, "energy", None, None)),
        check_vma=False,
    )
```

```python
import functools
import math

import jax
import jax.numpy as jnp
from jax import lax
from jax.experimental import pallas as pl
from jax.experimental.pallas import tpu as pltpu
from jax.sharding import PartitionSpec as P


VMEM = pltpu.MemorySpace.VMEM
SMEM = pltpu.MemorySpace.SMEM
HBM = pltpu.MemorySpace.HBM


def call(body, out_shape, spaces, *operands, scratch=()):
    several = isinstance(out_shape, (tuple, list))
    outs = out_shape if several else (out_shape,)
    held = sum(array.size * array.dtype.itemsize for array in (*operands, *outs))
    out_specs = [pl.BlockSpec(memory_space=VMEM) for _ in outs]
    return pl.pallas_call(
        body,
        out_shape=out_shape,
        in_specs=[pl.BlockSpec(memory_space=space) for space in spaces],
        out_specs=out_specs if several else out_specs[0],
        scratch_shapes=scratch,
        compiler_params=pltpu.CompilerParams(vmem_limit_bytes=2 * held + (4 << 20)),
    )(*operands)


def source_matrix(src_re, src_im):
    return jnp.concatenate(
        [
            jnp.concatenate([src_re, src_im], axis=1),
            jnp.concatenate([-src_im, src_re], axis=1),
        ],
        axis=0,
    )


def sandwich_block(block, source):
    half = block.shape[0]
    mid = jnp.dot(block, source, preferred_element_type=jnp.float32).astype(jnp.bfloat16)
    turned = jnp.concatenate([mid[:, half:], -mid[:, :half]], axis=1)
    left = jnp.concatenate([mid, turned], axis=0)
    return lax.dot_general(
        left, block, (((1,), (1,)), ((), ())), preferred_element_type=jnp.float32
    )


def prepare_kernel(coupling, screen, green, spectral, *rest):
    *blocks, diagonal, couple, sems = rest
    energy = lax.axis_index("energy")
    cell = lax.axis_index("cell")
    cells = screen.shape[2]
    owners, _, rows, _ = spectral.shape
    copies = [
        pltpu.make_async_copy(green.at[:, 0, cell], diagonal, sems.at[cells]),
        pltpu.make_async_copy(coupling, couple, sems.at[cells + 1]),
    ]
    for shift in range(cells):
        row = lax.rem(cell + shift, cells)
        copies.append(pltpu.make_async_copy(screen.at[:, 0, row], blocks[shift], sems.at[shift]))
    for copy in copies:
        copy.start()
    copies[0].wait()
    diag_re = diagonal[0].astype(jnp.float32)
    diag_im = diagonal[1].astype(jnp.float32)
    difference = (diag_re - diag_re.T, diag_im + diag_im.T)
    for owner in range(owners):
        for c in range(2):
            here = difference[c][owner * rows : (owner + 1) * rows]
            spectral[owner ^ energy, c] = here.astype(jnp.bfloat16)
    copies[1].wait()
    for shift in range(cells):
        copies[2 + shift].wait()
        weight = couple[lax.rem(cell + shift, cells), cell].astype(jnp.float32)
        blocks[shift][...] = (blocks[shift][...].astype(jnp.float32) * weight).astype(jnp.bfloat16)


def lesser_kernel(coupling, green, sigma, chunks):
    cell = lax.axis_index("cell")
    owners, cells, _, rows, _ = chunks.shape
    orbitals = owners * rows
    matrix = source_matrix(sigma[0, 0], sigma[1, 0])
    for i in range(cells):
        block = jnp.concatenate([green[0, 0, i], green[1, 0, i]], axis=1)
        part = sandwich_block(block, matrix)
        part = (part * coupling[i, cell].astype(jnp.float32)).astype(jnp.bfloat16)
        for owner in range(owners):
            for c in range(2):
                start = c * orbitals + owner * rows
                chunks[owner, i, c] = part[start : start + rows]


def correlate_kernel(chunks, spectral, polar):
    energies, cells = chunks.shape[0], chunks.shape[1]
    here = lax.axis_index("energy")
    scale = 1.0 / math.sqrt(energies)
    lesser, greater = [], []
    for e in range(energies):
        low, high = [], []
        for c in range(2):
            total = chunks[e, 0, c].astype(jnp.float32)
            for j in range(1, cells):
                total = total + chunks[e, j, c].astype(jnp.float32)
            above = total + spectral[here ^ e, c].astype(jnp.float32)
            low.append(total.astype(jnp.bfloat16).astype(jnp.float32))
            high.append(above.astype(jnp.bfloat16).astype(jnp.float32))
        lesser.append(low)
        greater.append(high)
    for w in range(energies):
        real = imag = None
        for e in range(energies - w):
            low_re, low_im = lesser[e + w]
            high_re, high_im = greater[e]
            re = low_im * high_re - low_re * high_im
            im = low_re * high_re + low_im * high_im
            real = re if real is None else real + re
            imag = im if imag is None else imag + im
        real = (real * scale).astype(jnp.bfloat16)
        imag = (imag * -scale).astype(jnp.bfloat16)
        for i in range(cells):
            polar[w, i, 0] = real
            polar[w, i, 1] = imag


def screened_kernel(_, rows, *rest):
    *blocks, polar, result = rest
    cell = lax.axis_index("cell")
    owners, cells, _, height, width = rows.shape
    total = None
    for shift in range(cells):
        j = lax.rem(cell + cells - shift, cells)
        parts = [rows[:, j, c].reshape(owners * height, width) for c in range(2)]
        if not shift:
            polar[0] = parts[0]
            polar[1] = parts[1]
        block = jnp.concatenate([blocks[shift][0], blocks[shift][1]], axis=1)
        part = sandwich_block(block, source_matrix(*parts))
        part = part.astype(jnp.bfloat16).astype(jnp.float32)
        total = part if total is None else total + part
    total = total.astype(jnp.bfloat16)
    result[0] = total[:width]
    result[1] = total[width:]


def spread_spectral(spectral, owners):
    held = [spectral[distance] for distance in range(owners)]
    bit = 1
    while bit < owners:
        moved = [distance for distance in range(owners) if distance & bit]
        sent = jnp.stack([held[distance] for distance in moved])
        got = lax.ppermute(sent, "energy", [(k, k ^ bit) for k in range(owners)])
        for place, distance in enumerate(moved):
            held[distance] = got[place]
        bit *= 2
    return jnp.stack(held)


def on_device(g_retarded, sigma_lesser, w_screened, coupling):
    owners = lax.axis_size("energy")
    cells = lax.axis_size("cell")
    orbitals = sigma_lesser.shape[2]
    rows = orbitals // owners
    half = functools.partial(jax.ShapeDtypeStruct, dtype=jnp.bfloat16)
    square = half((2, orbitals, orbitals))
    spectral, own, *leaving = call(
        prepare_kernel,
        (half((owners, 2, rows, orbitals)),) + (square,) * cells,
        (HBM, HBM, HBM),
        pltpu.with_memory_space_constraint(coupling, HBM),
        pltpu.with_memory_space_constraint(w_screened, HBM),
        pltpu.with_memory_space_constraint(g_retarded, HBM),
        scratch=(
            pltpu.VMEM(square.shape, square.dtype),
            pltpu.SMEM(coupling.shape, coupling.dtype),
            pltpu.SemaphoreType.DMA((cells + 2,)),
        ),
    )
    arrived = []
    for shift, block in enumerate(leaving, 1):
        pairs = [(k, (k + shift) % cells) for k in range(cells)]
        arrived.append(lax.ppermute(block, "cell", pairs))
    spectral = spread_spectral(spectral, owners)
    chunks = call(
        lesser_kernel,
        half((owners, cells, 2, rows, orbitals)),
        (SMEM, VMEM, VMEM),
        coupling,
        g_retarded,
        sigma_lesser,
    )
    chunks = lax.all_to_all(
        chunks.reshape(owners * cells, 2, rows, orbitals), ("energy", "cell"), 0, 0, tiled=True
    ).reshape(owners, cells, 2, rows, orbitals)
    polar = call(
        correlate_kernel,
        half((owners, cells, 2, rows, orbitals)),
        (VMEM, VMEM),
        chunks,
        spectral,
    )
    polar = lax.all_to_all(
        polar.reshape(owners * cells, 2, rows, orbitals), ("energy", "cell"), 0, 0, tiled=True
    ).reshape(owners, cells, 2, rows, orbitals)
    anchor = polar[0, 0, 0] * 2
    polar, screened = call(
        screened_kernel,
        (square, square),
        (HBM,) + (VMEM,) * (2 + len(arrived)),
        anchor,
        polar,
        own,
        *arrived,
    )
    return (
        polar.reshape(1, 2, 1, orbitals * orbitals),
        screened.reshape(1, 2, 1, orbitals, orbitals),
    )


def solution(mesh):
    return jax.shard_map(
        on_device,
        mesh=mesh,
        in_specs=(
            P(None, "energy", None, None, "cell"),
            P(None, "energy", None, "cell"),
            P(None, "energy", None, None, "cell"),
            P(),
        ),
        out_specs=(P("cell", None, "energy", None), P("cell", None, "energy", None, None)),
        check_vma=False,
    )
```

```python
import functools
import math

import jax
import jax.numpy as jnp
from jax import lax
from jax.experimental import pallas as pl
from jax.experimental.pallas import tpu as pltpu
from jax.sharding import PartitionSpec as P


VMEM = pltpu.MemorySpace.VMEM
HBM = pltpu.MemorySpace.HBM


def call(body, out_shape, spaces, *operands, scratch=(), out_spaces=None):
    several = isinstance(out_shape, (tuple, list))
    outs = out_shape if several else (out_shape,)
    held = sum(array.size * array.dtype.itemsize for array in (*operands, *outs))
    out_specs = [
        pl.BlockSpec(memory_space=space) for space in out_spaces or (VMEM,) * len(outs)
    ]
    return pl.pallas_call(
        body,
        out_shape=out_shape,
        in_specs=[pl.BlockSpec(memory_space=space) for space in spaces],
        out_specs=out_specs if several else out_specs[0],
        scratch_shapes=scratch,
        compiler_params=pltpu.CompilerParams(vmem_limit_bytes=2 * held + (4 << 20)),
    )(*operands)


def partner(cell, shift, cells):
    if cells & (cells - 1) == 0:
        return cell ^ abs(shift)
    return (cell + shift + cells) % cells


def source_matrix(src_re, src_im):
    return jnp.concatenate(
        [
            jnp.concatenate([src_re, src_im], axis=1),
            jnp.concatenate([-src_im, src_re], axis=1),
        ],
        axis=0,
    )


def sandwich_block(block, source):
    half = block.shape[0]
    mid = jnp.dot(block, source, preferred_element_type=jnp.float32).astype(jnp.bfloat16)
    turned = jnp.concatenate([-block[:, half:], block[:, :half]], axis=1)
    right = jnp.concatenate([block, turned], axis=0)
    both = lax.dot_general(
        mid, right, (((1,), (1,)), ((), ())), preferred_element_type=jnp.float32
    )
    return jnp.concatenate([both[:, :half], both[:, half:]], axis=0)


def lesser_kernel(coupling, screen, green, sigma, chunks, spectral, *rest):
    cells = screen.shape[2]
    blocks, (couple, source, columns, placed, arrivals, departures) = rest[:cells], rest[cells:]
    energy = lax.axis_index("energy")
    cell = lax.axis_index("cell")
    owners, _, rows, orbitals = spectral.shape
    copies = [
        pltpu.make_async_copy(coupling, couple, arrivals.at[0]),
        pltpu.make_async_copy(sigma.at[:, 0], source, arrivals.at[1]),
        pltpu.make_async_copy(green.at[:, 0], columns, arrivals.at[2]),
    ]
    for shift in range(cells):
        row = partner(cell, shift, cells)
        copies.append(
            pltpu.make_async_copy(screen.at[:, 0, row], blocks[shift], arrivals.at[3 + shift])
        )
    for copy in copies:
        copy.start()
    for copy in copies[:3]:
        copy.wait()
    matrix = source_matrix(source[0], source[1])
    leaving = []
    for i in range(cells):
        block = jnp.concatenate([columns[0, i], columns[1, i]], axis=1)
        part = sandwich_block(block, matrix)
        part = (part * couple[i, cell].astype(jnp.float32)).astype(jnp.bfloat16)
        for owner in range(owners):
            for c in range(2):
                start = c * orbitals + owner * rows
                placed[i, owner, c] = part[start : start + rows]
        leaving.append(pltpu.make_async_copy(placed.at[i], chunks.at[:, i], departures.at[i]))
        leaving[-1].start()
    diag_re = columns[0, cell].astype(jnp.float32)
    diag_im = columns[1, cell].astype(jnp.float32)
    difference = (diag_re - diag_re.T, diag_im + diag_im.T)
    for owner in range(owners):
        for c in range(2):
            here = difference[c][owner * rows : (owner + 1) * rows]
            spectral[owner ^ energy, c] = here.astype(jnp.bfloat16)
    for shift in range(cells):
        copies[3 + shift].wait()
        weight = couple[partner(cell, shift, cells), cell].astype(jnp.float32)
        blocks[shift][...] = (blocks[shift][...].astype(jnp.float32) * weight).astype(jnp.bfloat16)
    for copy in leaving:
        copy.wait()


def correlate_kernel(chunks, spectral, polar):
    energies, cells = chunks.shape[0], chunks.shape[1]
    here = lax.axis_index("energy")
    scale = 1.0 / math.sqrt(energies)
    lesser, greater = [], []
    for e in range(energies):
        low, high = [], []
        for c in range(2):
            total = chunks[e, 0, c].astype(jnp.float32)
            for j in range(1, cells):
                total = total + chunks[e, j, c].astype(jnp.float32)
            above = total + spectral[here ^ e, c].astype(jnp.float32)
            low.append(total.astype(jnp.bfloat16).astype(jnp.float32))
            high.append(above.astype(jnp.bfloat16).astype(jnp.float32))
        lesser.append(low)
        greater.append(high)
    for w in range(energies):
        real = imag = None
        for e in range(energies - w):
            low_re, low_im = lesser[e + w]
            high_re, high_im = greater[e]
            re = low_im * high_re - low_re * high_im
            im = low_re * high_re + low_im * high_im
            real = re if real is None else real + re
            imag = im if imag is None else imag + im
        real = (real * scale).astype(jnp.bfloat16)
        imag = (imag * -scale).astype(jnp.bfloat16)
        for i in range(cells):
            polar[w, i, 0] = real
            polar[w, i, 1] = imag


def screened_kernel(_, rows, *rest):
    *blocks, polar, result = rest
    cell = lax.axis_index("cell")
    owners, cells, _, height, width = rows.shape
    total = None
    for shift in range(cells):
        j = partner(cell, -shift, cells)
        parts = [rows[:, j, c].reshape(owners * height, width) for c in range(2)]
        if not shift:
            polar[...] = jnp.stack(parts, axis=1)
        block = jnp.concatenate([blocks[shift][0], blocks[shift][1]], axis=1)
        part = sandwich_block(block, source_matrix(*parts))
        part = part.astype(jnp.bfloat16).astype(jnp.float32)
        total = part if total is None else total + part
    total = total.astype(jnp.bfloat16)
    result[0] = total[:width]
    result[1] = total[width:]


def spread_spectral(spectral, owners):
    held = [spectral[distance] for distance in range(owners)]
    bit = 1
    while bit < owners:
        moved = [distance for distance in range(owners) if distance & bit]
        sent = jnp.stack([held[distance] for distance in moved])
        got = lax.ppermute(sent, "energy", [(k, k ^ bit) for k in range(owners)])
        for place, distance in enumerate(moved):
            held[distance] = got[place]
        bit *= 2
    return jnp.stack(held)


def on_device(g_retarded, sigma_lesser, w_screened, coupling):
    owners = lax.axis_size("energy")
    cells = lax.axis_size("cell")
    orbitals = sigma_lesser.shape[2]
    rows = orbitals // owners
    half = functools.partial(jax.ShapeDtypeStruct, dtype=jnp.bfloat16)
    square = half((2, orbitals, orbitals))
    chunks, spectral, own, *leaving = call(
        lesser_kernel,
        (half((owners, cells, 2, rows, orbitals)), half((owners, 2, rows, orbitals)))
        + (square,) * cells,
        (HBM,) * 4,
        *(
            pltpu.with_memory_space_constraint(array, HBM)
            for array in (coupling, w_screened, g_retarded, sigma_lesser)
        ),
        scratch=(
            pltpu.SMEM(coupling.shape, coupling.dtype),
            pltpu.VMEM(square.shape, square.dtype),
            pltpu.VMEM((2, cells, orbitals, orbitals), jnp.bfloat16),
            pltpu.VMEM((cells, owners, 2, rows, orbitals), jnp.bfloat16),
            pltpu.SemaphoreType.DMA((cells + 3,)),
            pltpu.SemaphoreType.DMA((cells,)),
        ),
        out_spaces=(HBM,) + (VMEM,) * (cells + 1),
    )
    arrived = []
    for shift, block in enumerate(leaving, 1):
        pairs = [(k, partner(k, shift, cells)) for k in range(cells)]
        arrived.append(lax.ppermute(block, "cell", pairs))
    spectral = spread_spectral(spectral, owners)
    chunks = lax.all_to_all(
        chunks.reshape(owners * cells, 2, rows, orbitals), ("energy", "cell"), 0, 0, tiled=True
    ).reshape(owners, cells, 2, rows, orbitals)
    polar = call(
        correlate_kernel,
        half((owners, cells, 2, rows, orbitals)),
        (VMEM, VMEM),
        chunks,
        spectral,
    )
    polar = lax.all_to_all(
        polar.reshape(owners * cells, 2, rows, orbitals), ("energy", "cell"), 0, 0, tiled=True
    ).reshape(owners, cells, 2, rows, orbitals)
    anchor = polar[0, 0, 0] * 2
    polar, screened = call(
        screened_kernel,
        (half((orbitals, 2, orbitals)), square),
        (HBM,) + (VMEM,) * (2 + len(arrived)),
        anchor,
        polar,
        own,
        *arrived,
    )
    return (
        jnp.swapaxes(polar, 0, 1).reshape(1, 2, 1, orbitals * orbitals),
        screened.reshape(1, 2, 1, orbitals, orbitals),
    )


def solution(mesh):
    return jax.shard_map(
        on_device,
        mesh=mesh,
        in_specs=(
            P(None, "energy", None, None, "cell"),
            P(None, "energy", None, "cell"),
            P(None, "energy", None, None, "cell"),
            P(),
        ),
        out_specs=(P("cell", None, "energy", None), P("cell", None, "energy", None, None)),
        check_vma=False,
    )
```

```python
import functools
import math

import jax
import jax.numpy as jnp
from jax import lax
from jax.experimental import pallas as pl
from jax.experimental.pallas import tpu as pltpu
from jax.sharding import PartitionSpec as P


VMEM = pltpu.MemorySpace.VMEM
HBM = pltpu.MemorySpace.HBM


def call(body, out_shape, spaces, *operands, scratch=(), out_spaces=None):
    several = isinstance(out_shape, (tuple, list))
    outs = out_shape if several else (out_shape,)
    held = sum(array.size * array.dtype.itemsize for array in (*operands, *outs))
    out_specs = [
        pl.BlockSpec(memory_space=space) for space in out_spaces or (VMEM,) * len(outs)
    ]
    return pl.pallas_call(
        body,
        out_shape=out_shape,
        in_specs=[pl.BlockSpec(memory_space=space) for space in spaces],
        out_specs=out_specs if several else out_specs[0],
        scratch_shapes=scratch,
        compiler_params=pltpu.CompilerParams(vmem_limit_bytes=2 * held + (4 << 20)),
    )(*operands)


def partner(cell, shift, cells):
    if cells & (cells - 1) == 0:
        return cell ^ abs(shift)
    return (cell + shift + cells) % cells


def source_matrix(src_re, src_im):
    return jnp.concatenate(
        [
            jnp.concatenate([src_re, src_im], axis=1),
            jnp.concatenate([-src_im, src_re], axis=1),
        ],
        axis=0,
    )


def sandwich_block(block, source):
    half = block.shape[0]
    mid = jnp.dot(block, source, preferred_element_type=jnp.float32).astype(jnp.bfloat16)
    turned = jnp.concatenate([-block[:, half:], block[:, :half]], axis=1)
    right = jnp.concatenate([block, turned], axis=0)
    both = lax.dot_general(
        mid, right, (((1,), (1,)), ((), ())), preferred_element_type=jnp.float32
    )
    return jnp.concatenate([both[:, :half], both[:, half:]], axis=0)


def lesser_kernel(coupling, screen, green, sigma, chunks, spectral, *rest):
    cells = screen.shape[2]
    blocks, (couple, source, columns, placed, arrivals, departures) = rest[:cells], rest[cells:]
    energy = lax.axis_index("energy")
    cell = lax.axis_index("cell")
    owners, _, rows, orbitals = spectral.shape
    copies = [
        pltpu.make_async_copy(coupling, couple, arrivals.at[0]),
        pltpu.make_async_copy(sigma.at[:, 0], source, arrivals.at[1]),
        pltpu.make_async_copy(green.at[:, 0], columns, arrivals.at[2]),
    ]
    for shift in range(cells):
        row = partner(cell, shift, cells)
        copies.append(
            pltpu.make_async_copy(screen.at[:, 0, row], blocks[shift], arrivals.at[3 + shift])
        )
    for copy in copies:
        copy.start()
    for copy in copies[:3]:
        copy.wait()
    matrix = source_matrix(source[0], source[1])
    leaving = []
    for i in range(cells):
        block = jnp.concatenate([columns[0, i], columns[1, i]], axis=1)
        part = sandwich_block(block, matrix)
        part = (part * couple[i, cell].astype(jnp.float32)).astype(jnp.bfloat16)
        for owner in range(owners):
            for c in range(2):
                start = c * orbitals + owner * rows
                placed[i, owner, c] = part[start : start + rows]
        leaving.append(pltpu.make_async_copy(placed.at[i], chunks.at[:, i], departures.at[i]))
        leaving[-1].start()
    diag_re = columns[0, cell].astype(jnp.float32)
    diag_im = columns[1, cell].astype(jnp.float32)
    difference = (diag_re - diag_re.T, diag_im + diag_im.T)
    for owner in range(owners):
        for c in range(2):
            here = difference[c][owner * rows : (owner + 1) * rows]
            spectral[owner ^ energy, c] = here.astype(jnp.bfloat16)
    for shift in range(cells):
        copies[3 + shift].wait()
        weight = couple[partner(cell, shift, cells), cell].astype(jnp.float32)
        blocks[shift][...] = (blocks[shift][...].astype(jnp.float32) * weight).astype(jnp.bfloat16)
    for copy in leaving:
        copy.wait()


def correlate_kernel(chunks, spectral, polar):
    energies, cells = chunks.shape[0], chunks.shape[1]
    here = lax.axis_index("energy")
    scale = 1.0 / math.sqrt(energies)
    lesser, greater = [], []
    for e in range(energies):
        low, high = [], []
        for c in range(2):
            total = chunks[e, 0, c].astype(jnp.float32)
            for j in range(1, cells):
                total = total + chunks[e, j, c].astype(jnp.float32)
            above = total + spectral[here ^ e, c].astype(jnp.float32)
            low.append(total.astype(jnp.bfloat16).astype(jnp.float32))
            high.append(above.astype(jnp.bfloat16).astype(jnp.float32))
        lesser.append(low)
        greater.append(high)
    for w in range(energies):
        real = imag = None
        for e in range(energies - w):
            low_re, low_im = lesser[e + w]
            high_re, high_im = greater[e]
            re = low_im * high_re - low_re * high_im
            im = low_re * high_re + low_im * high_im
            real = re if real is None else real + re
            imag = im if imag is None else imag + im
        real = (real * scale).astype(jnp.bfloat16)
        imag = (imag * -scale).astype(jnp.bfloat16)
        for i in range(cells):
            polar[w, i, 0] = real
            polar[w, i, 1] = imag


def screened_kernel(_, rows, *rest):
    *blocks, polar, result = rest
    cell = lax.axis_index("cell")
    owners, cells, _, height, width = rows.shape
    total = None
    for shift in range(cells):
        j = partner(cell, -shift, cells)
        parts = [rows[:, j, c].reshape(owners * height, width) for c in range(2)]
        if not shift:
            polar[...] = jnp.stack(parts, axis=1)
        block = jnp.concatenate([blocks[shift][0], blocks[shift][1]], axis=1)
        part = sandwich_block(block, source_matrix(*parts))
        part = part.astype(jnp.bfloat16).astype(jnp.float32)
        total = part if total is None else total + part
    total = total.astype(jnp.bfloat16)
    result[0] = total[:width]
    result[1] = total[width:]


def spread_spectral(spectral, owners):
    held = [spectral[distance] for distance in range(owners)]

    def exchange(moved, mask):
        sent = jnp.stack([held[distance] for distance in moved])
        got = lax.ppermute(sent, "energy", [(k, k ^ mask) for k in range(owners)])
        for place, distance in enumerate(moved):
            held[distance] = got[place]

    exchange(range(1, owners, 2), 1)
    for mask in range(2, owners, 2):
        exchange((mask, mask + 1), mask)
    return jnp.stack(held)


def on_device(g_retarded, sigma_lesser, w_screened, coupling):
    owners = lax.axis_size("energy")
    cells = lax.axis_size("cell")
    orbitals = sigma_lesser.shape[2]
    rows = orbitals // owners
    half = functools.partial(jax.ShapeDtypeStruct, dtype=jnp.bfloat16)
    square = half((2, orbitals, orbitals))
    chunks, spectral, own, *leaving = call(
        lesser_kernel,
        (half((owners, cells, 2, rows, orbitals)), half((owners, 2, rows, orbitals)))
        + (square,) * cells,
        (HBM,) * 4,
        *(
            pltpu.with_memory_space_constraint(array, HBM)
            for array in (coupling, w_screened, g_retarded, sigma_lesser)
        ),
        scratch=(
            pltpu.SMEM(coupling.shape, coupling.dtype),
            pltpu.VMEM(square.shape, square.dtype),
            pltpu.VMEM((2, cells, orbitals, orbitals), jnp.bfloat16),
            pltpu.VMEM((cells, owners, 2, rows, orbitals), jnp.bfloat16),
            pltpu.SemaphoreType.DMA((cells + 3,)),
            pltpu.SemaphoreType.DMA((cells,)),
        ),
        out_spaces=(HBM,) + (VMEM,) * (cells + 1),
    )
    arrived = []
    for shift, block in enumerate(leaving, 1):
        pairs = [(k, partner(k, shift, cells)) for k in range(cells)]
        arrived.append(lax.ppermute(block, "cell", pairs))
    spectral = spread_spectral(spectral, owners)
    chunks = lax.all_to_all(
        chunks.reshape(owners * cells, 2, rows, orbitals), ("energy", "cell"), 0, 0, tiled=True
    ).reshape(owners, cells, 2, rows, orbitals)
    polar = call(
        correlate_kernel,
        half((owners, cells, 2, rows, orbitals)),
        (VMEM, VMEM),
        chunks,
        spectral,
    )
    polar = lax.all_to_all(
        polar.reshape(owners * cells, 2, rows, orbitals), ("energy", "cell"), 0, 0, tiled=True
    ).reshape(owners, cells, 2, rows, orbitals)
    anchor = polar[0, 0, 0] * 2
    polar, screened = call(
        screened_kernel,
        (half((orbitals, 2, orbitals)), square),
        (HBM,) + (VMEM,) * (2 + len(arrived)),
        anchor,
        polar,
        own,
        *arrived,
    )
    return (
        jnp.swapaxes(polar, 0, 1).reshape(1, 2, 1, orbitals * orbitals),
        screened.reshape(1, 2, 1, orbitals, orbitals),
    )


def solution(mesh):
    return jax.shard_map(
        on_device,
        mesh=mesh,
        in_specs=(
            P(None, "energy", None, None, "cell"),
            P(None, "energy", None, "cell"),
            P(None, "energy", None, None, "cell"),
            P(),
        ),
        out_specs=(P("cell", None, "energy", None), P("cell", None, "energy", None, None)),
        check_vma=False,
    )
```

```python
import functools
import math

import jax
import jax.numpy as jnp
from jax import lax
from jax.experimental import pallas as pl
from jax.experimental.pallas import tpu as pltpu
from jax.sharding import PartitionSpec as P


VMEM = pltpu.MemorySpace.VMEM
HBM = pltpu.MemorySpace.HBM


def call(body, out_shape, spaces, *operands, scratch=(), out_spaces=None):
    several = isinstance(out_shape, (tuple, list))
    outs = out_shape if several else (out_shape,)
    held = sum(array.size * array.dtype.itemsize for array in (*operands, *outs))
    out_specs = [
        pl.BlockSpec(memory_space=space) for space in out_spaces or (VMEM,) * len(outs)
    ]
    return pl.pallas_call(
        body,
        out_shape=out_shape,
        in_specs=[pl.BlockSpec(memory_space=space) for space in spaces],
        out_specs=out_specs if several else out_specs[0],
        scratch_shapes=scratch,
        compiler_params=pltpu.CompilerParams(vmem_limit_bytes=2 * held + (4 << 20)),
    )(*operands)


def partner(cell, shift, cells):
    if cells & (cells - 1) == 0:
        return cell ^ abs(shift)
    return (cell + shift + cells) % cells


def source_matrix(src_re, src_im):
    return jnp.concatenate(
        [
            jnp.concatenate([src_re, src_im], axis=1),
            jnp.concatenate([-src_im, src_re], axis=1),
        ],
        axis=0,
    )


def sandwich_block(block, source):
    half = block.shape[0]
    mid = jnp.dot(block, source, preferred_element_type=jnp.float32).astype(jnp.bfloat16)
    turned = jnp.concatenate([-block[:, half:], block[:, :half]], axis=1)
    right = jnp.concatenate([block, turned], axis=0)
    both = lax.dot_general(
        mid, right, (((1,), (1,)), ((), ())), preferred_element_type=jnp.float32
    )
    return jnp.concatenate([both[:, :half], both[:, half:]], axis=0)


def lesser_kernel(coupling, screen, green, sigma, chunks, spectral, *rest):
    cells = screen.shape[2]
    blocks, (couple, source, columns, placed, arrivals, departures) = rest[:cells], rest[cells:]
    energy = lax.axis_index("energy")
    cell = lax.axis_index("cell")
    owners, _, rows, orbitals = spectral.shape
    copies = [
        pltpu.make_async_copy(coupling, couple, arrivals.at[0]),
        pltpu.make_async_copy(sigma.at[:, 0], source, arrivals.at[1]),
        pltpu.make_async_copy(green.at[:, 0], columns, arrivals.at[2]),
    ]
    for shift in range(cells):
        row = partner(cell, shift, cells)
        copies.append(
            pltpu.make_async_copy(screen.at[:, 0, row], blocks[shift], arrivals.at[3 + shift])
        )
    for copy in copies:
        copy.start()
    for copy in copies[:3]:
        copy.wait()
    matrix = source_matrix(source[0], source[1])
    leaving = []
    for i in range(cells):
        block = jnp.concatenate([columns[0, i], columns[1, i]], axis=1)
        part = sandwich_block(block, matrix)
        part = (part * couple[i, cell].astype(jnp.float32)).astype(jnp.bfloat16)
        for owner in range(owners):
            for c in range(2):
                start = c * orbitals + owner * rows
                placed[i, owner, c] = part[start : start + rows]
        leaving.append(pltpu.make_async_copy(placed.at[i], chunks.at[:, i], departures.at[i]))
        leaving[-1].start()
    diag_re = columns[0, cell].astype(jnp.float32)
    diag_im = columns[1, cell].astype(jnp.float32)
    difference = (diag_re - diag_re.T, diag_im + diag_im.T)
    for owner in range(owners):
        for c in range(2):
            here = difference[c][owner * rows : (owner + 1) * rows]
            spectral[owner ^ energy, c] = here
    for shift in range(cells):
        copies[3 + shift].wait()
        weight = couple[partner(cell, shift, cells), cell].astype(jnp.float32)
        blocks[shift][...] = (blocks[shift][...].astype(jnp.float32) * weight).astype(jnp.bfloat16)
    for copy in leaving:
        copy.wait()


def correlate_kernel(chunks, spectral, polar):
    energies, cells = chunks.shape[0], chunks.shape[1]
    here = lax.axis_index("energy")
    scale = 1.0 / math.sqrt(energies)
    lesser, greater = [], []
    for e in range(energies):
        low, high = [], []
        for c in range(2):
            total = chunks[e, 0, c].astype(jnp.float32)
            for j in range(1, cells):
                total = total + chunks[e, j, c].astype(jnp.float32)
            above = total + spectral[here ^ e, c]
            low.append(total.astype(jnp.bfloat16).astype(jnp.float32))
            high.append(above.astype(jnp.bfloat16).astype(jnp.float32))
        lesser.append(low)
        greater.append(high)
    for w in range(energies):
        real = imag = None
        for e in range(energies - w):
            low_re, low_im = lesser[e + w]
            high_re, high_im = greater[e]
            re = low_im * high_re - low_re * high_im
            im = low_re * high_re + low_im * high_im
            real = re if real is None else real + re
            imag = im if imag is None else imag + im
        real = (real * scale).astype(jnp.bfloat16)
        imag = (imag * -scale).astype(jnp.bfloat16)
        for i in range(cells):
            polar[w, i, 0] = real
            polar[w, i, 1] = imag


def screened_kernel(_, rows, *rest):
    *blocks, polar, result = rest
    cell = lax.axis_index("cell")
    owners, cells, _, height, width = rows.shape
    total = None
    for shift in range(cells):
        j = partner(cell, -shift, cells)
        parts = [rows[:, j, c].reshape(owners * height, width) for c in range(2)]
        if not shift:
            polar[...] = jnp.stack(parts, axis=1)
        block = jnp.concatenate([blocks[shift][0], blocks[shift][1]], axis=1)
        part = sandwich_block(block, source_matrix(*parts))
        part = part.astype(jnp.bfloat16).astype(jnp.float32)
        total = part if total is None else total + part
    total = total.astype(jnp.bfloat16)
    result[0] = total[:width]
    result[1] = total[width:]


def spread_spectral(spectral, owners):
    held = [spectral[distance] for distance in range(owners)]

    def exchange(moved, mask):
        sent = jnp.stack([held[distance] for distance in moved])
        got = lax.ppermute(sent, "energy", [(k, k ^ mask) for k in range(owners)])
        for place, distance in enumerate(moved):
            held[distance] = got[place]

    exchange(range(1, owners, 2), 1)
    for mask in range(2, owners, 2):
        exchange((mask, mask + 1), mask)
    return jnp.stack(held)


def on_device(g_retarded, sigma_lesser, w_screened, coupling):
    owners = lax.axis_size("energy")
    cells = lax.axis_size("cell")
    orbitals = sigma_lesser.shape[2]
    rows = orbitals // owners
    half = functools.partial(jax.ShapeDtypeStruct, dtype=jnp.bfloat16)
    square = half((2, orbitals, orbitals))
    chunks, spectral, own, *leaving = call(
        lesser_kernel,
        (
            half((owners, cells, 2, rows, orbitals)),
            jax.ShapeDtypeStruct((owners, 2, rows, orbitals), jnp.float32),
        )
        + (square,) * cells,
        (HBM,) * 4,
        *(
            pltpu.with_memory_space_constraint(array, HBM)
            for array in (coupling, w_screened, g_retarded, sigma_lesser)
        ),
        scratch=(
            pltpu.SMEM(coupling.shape, coupling.dtype),
            pltpu.VMEM(square.shape, square.dtype),
            pltpu.VMEM((2, cells, orbitals, orbitals), jnp.bfloat16),
            pltpu.VMEM((cells, owners, 2, rows, orbitals), jnp.bfloat16),
            pltpu.SemaphoreType.DMA((cells + 3,)),
            pltpu.SemaphoreType.DMA((cells,)),
        ),
        out_spaces=(HBM,) + (VMEM,) * (cells + 1),
    )
    arrived = []
    for shift, block in enumerate(leaving, 1):
        pairs = [(k, partner(k, shift, cells)) for k in range(cells)]
        arrived.append(lax.ppermute(block, "cell", pairs))
    spectral = spread_spectral(spectral, owners)
    chunks = lax.all_to_all(
        chunks.reshape(owners * cells, 2, rows, orbitals), ("energy", "cell"), 0, 0, tiled=True
    ).reshape(owners, cells, 2, rows, orbitals)
    polar = call(
        correlate_kernel,
        half((owners, cells, 2, rows, orbitals)),
        (VMEM, VMEM),
        chunks,
        spectral,
    )
    polar = lax.all_to_all(
        polar.reshape(owners * cells, 2, rows, orbitals), ("energy", "cell"), 0, 0, tiled=True
    ).reshape(owners, cells, 2, rows, orbitals)
    anchor = polar[0, 0, 0] * 2
    polar, screened = call(
        screened_kernel,
        (half((orbitals, 2, orbitals)), square),
        (HBM,) + (VMEM,) * (2 + len(arrived)),
        anchor,
        polar,
        own,
        *arrived,
    )
    return (
        jnp.swapaxes(polar, 0, 1).reshape(1, 2, 1, orbitals * orbitals),
        screened.reshape(1, 2, 1, orbitals, orbitals),
    )


def solution(mesh):
    return jax.shard_map(
        on_device,
        mesh=mesh,
        in_specs=(
            P(None, "energy", None, None, "cell"),
            P(None, "energy", None, "cell"),
            P(None, "energy", None, None, "cell"),
            P(),
        ),
        out_specs=(P("cell", None, "energy", None), P("cell", None, "energy", None, None)),
        check_vma=False,
    )
```
